256 devices in a mesh: gx: 4 (over x), gy: 16 (over z, core), gz: 4 (over y).
Axes of the slice: x: 4, y: 4, z: 8, core: 2. Of those that a mesh axis runs over, the one named last changes fastest.
Arguments:
- volume: float32 [512, 1024, 512], P('gx', 'gy', 'gz'), may hold values from -6 to 6
Outputs:
- prefix: float32 [512, 1024, 512], P('gx', 'gy', 'gz')
- box_sum: float32 [512, 1024, 512], P('gx', 'gy', 'gz')
The draws below stay inside these ranges and needn't reach their ends.
All inputs are finite; a program needn't handle non-finite values.
Results may differ from the reference program's by a relative error of at most 0.00055.
Values sent between devices are 32-bit elements; how exact they have to be, the bound alone decides.
No kernel may reach another device: no remote copies, remote signals or barrier semaphores. Data moves between devices by JAX's collectives and lax.ppermute only.
A program may use at most 128 MiB of HBM per device.

```python
import math
import jax
import jax.numpy as jnp

NX = 512
NY = 1024
NZ = 512


def level_of(own_key, shape, split, least, high):
    factor_of = 1.0
    for axis_at, shards_of in split:
        draws = jax.random.uniform(jax.random.fold_in(jax.random.fold_in(own_key, 6), axis_at), (shards_of,), jnp.float32, least / len(split), high / len(split))
        factor_of = factor_of * jnp.repeat(jnp.exp(draws), shape[axis_at] // shards_of).reshape((-1,) + (1,) * (len(shape) - 1 - axis_at))
    return factor_of


def normal_values(stream_key, dims, deviation, bound, pieces=(), dtype=jnp.bfloat16):
    result = jax.random.normal(stream_key, dims, jnp.float32) * deviation
    if len(pieces) > 0:
        result = level_of(stream_key, dims, pieces, -0.22, 0.18) * result
    return jnp.clip(result, min=-bound, max=bound).astype(dtype)


def setup_inputs(seed: int = 0) -> dict:
    key_of = jax.random.split(jax.random.key(seed), 2)
    volume = normal_values(key_of[0], (NX, NY, NZ), 1.0, 6.0, ((0, 4), (1, 16), (2, 4)), jnp.float32)
    return {"volume": volume}


def reference(volume):
    summed = jnp.cumsum(jnp.cumsum(jnp.cumsum(volume, axis=2), axis=1), axis=0)
    size_x, size_y, size_z = volume.shape
    prefix = summed * jnp.float32(1.0 / math.sqrt(size_x * size_y * size_z))
    padded = jnp.pad(summed, ((3, 0), (3, 0), (3, 0)))
    padded = jnp.pad(padded, ((0, 2), (0, 2), (0, 2)), mode='edge')
    total = jnp.zeros(volume.shape, jnp.float32)
    for first in range(2):
        for second in range(2):
            for third in range(2):
                piece = padded[5 * first:5 * first + size_x, 5 * second:5 * second + size_y, 5 * third:5 * third + size_z]
                if (3 - first - second - third) % 2 == 0:
                    total = total + piece
                else:
                    total = total - piece
    box_sum = total * jnp.float32(1.0 / math.sqrt(125.0))
    return (prefix, box_sum)
```

```python
import functools
import math

import jax
import jax.numpy as jnp
from jax import lax
from jax.experimental import pallas as pl
from jax.experimental.pallas import tpu as pltpu
from jax.sharding import PartitionSpec as P


F32, BF16 = jnp.float32, jnp.bfloat16
MIB = 1 << 20


def iota(shape, dim):
    return lax.broadcasted_iota(jnp.int32, shape, dim)


def split(v):
    high = v.astype(BF16)
    return high, (v - high.astype(F32)).astype(BF16)


def ones_where(keep):
    return jnp.where(keep, 1.0, 0.0).astype(BF16)


def times(v, ones):
    high, low = split(v)
    dot = functools.partial(jnp.dot, preferred_element_type=F32)
    return dot(high, ones) + dot(low, ones)


def times_left(ones, v):
    high, low = split(v)
    dot = functools.partial(jnp.dot, preferred_element_type=F32)
    return dot(ones, high) + dot(ones, low)


def upper(n):
    return ones_where(iota((n, n), 0) <= iota((n, n), 1))


def lower(n):
    return ones_where(iota((n, n), 1) <= iota((n, n), 0))


def scan_rows(v):
    dim, n = v.ndim - 2, v.shape[-2]
    step = 1
    while step < n:
        if step < 8:
            moved = jnp.where(iota(v.shape, dim) >= step, pltpu.roll(v, step, dim), 0.0)
        else:
            kept = lax.slice_in_dim(v, 0, n - step, axis=dim)
            moved = jnp.concatenate([jnp.zeros_like(lax.slice_in_dim(v, 0, step, axis=dim)), kept], axis=dim)
        v = v + moved
        step *= 2
    return v


def five_rows(v):
    n = v.shape[0]
    two = v[: n - 1] + v[1:]
    four = two[: n - 3] + two[2:]
    return four[: n - 4] + v[4:]


def cost(flops, moved):
    return pl.CostEstimate(flops=flops, bytes_accessed=moved, transcendentals=0)


def call(body, out, grid=None, ins=None, outs=None, scratch=(), flops=1 << 20, moved=1 << 20, vmem=24):
    shapes = [jax.ShapeDtypeStruct(s, F32) for s in out]
    kw = {}
    if grid is not None:
        kw = dict(grid=grid, in_specs=ins, out_specs=outs)
    return pl.pallas_call(
        body,
        out_shape=shapes,
        scratch_shapes=list(scratch),
        compiler_params=pltpu.CompilerParams(vmem_limit_bytes=vmem * MIB),
        cost_estimate=cost(flops, moved),
        **kw,
    )


def whole(shape):
    return pl.BlockSpec(shape, lambda *_: (0,) * len(shape))


def totals_body(pieces, v_ref, held_ref, rz_ref, rx_ref, ry_ref, sems):
    nx, ny, nz = held_ref.shape
    n = nx // pieces
    copies = [
        pltpu.make_async_copy(v_ref.at[pl.ds(k * n, n)], held_ref.at[pl.ds(k * n, n)], sems.at[k]) for k in range(pieces)
    ]
    for copy in copies:
        copy.start()
    lane = iota((ny, nx), 1)

    def group(i, carry):
        rz, rx = carry
        rows = []
        for j in range(8):
            v = held_ref[i * 8 + j]
            rx = rx + v
            rows.append(jnp.sum(v, axis=0, keepdims=True))
            rz = jnp.where(lane == i * 8 + j, jnp.sum(v, axis=1, keepdims=True), rz)
        ry_ref[pl.ds(pl.multiple_of(i * 8, 8), 8), :] = jnp.concatenate(rows, axis=0)
        return rz, rx

    carry = jnp.zeros((ny, nx), F32), jnp.zeros((ny, nz), F32)
    for k, copy in enumerate(copies):
        copy.wait()
        carry = lax.fori_loop(k * n // 8, (k + 1) * n // 8, group, carry)
    rz_ref[...], rx_ref[...] = carry


def totals(v):
    nx, ny, nz = v.shape
    pieces = 4
    out = [v.shape, (ny, nx), (ny, nz), (nx, nz)]
    return pl.pallas_call(
        functools.partial(totals_body, pieces),
        out_shape=[jax.ShapeDtypeStruct(s, F32) for s in out],
        in_specs=[pl.BlockSpec(memory_space=pltpu.HBM)],
        out_specs=[pl.BlockSpec(memory_space=pltpu.VMEM)] * 4,
        scratch_shapes=[pltpu.SemaphoreType.DMA((pieces,))],
        compiler_params=pltpu.CompilerParams(vmem_limit_bytes=24 * MIB),
        cost_estimate=cost(6 << 20, 8 << 20),
    )(v)


def lower_sum(own, parts):
    total = jnp.where(own >= 1, parts[0][...], 0.0)
    for d in range(1, len(parts)):
        total = total + jnp.where(own >= d + 1, parts[d][...], 0.0)
    return total


def after_z_body(r1, r2, r3, rx_ref, cz_ref, out_ref):
    cz = lower_sum(lax.axis_index("gz"), (r1, r2, r3))
    cz_ref[...] = cz
    rx = rx_ref[...]
    out_ref[...] = rx + jnp.where(iota(rx.shape, 1) == 0, jnp.sum(cz, axis=1, keepdims=True), 0.0)


def after_x_body(r1, r2, r3, cz_ref, ry_ref, cx_ref, out_ref):
    cx = lower_sum(lax.axis_index("gx"), (r1, r2, r3))
    cx_ref[...] = cx
    ry = ry_ref[...]
    n = ry.shape[0]
    row = jnp.sum(cz_ref[...], axis=0, keepdims=True)
    column = jnp.sum(jnp.where(iota((n, n), 0) == iota((n, n), 1), row, 0.0), axis=1, keepdims=True)
    ry = ry + jnp.where(iota(ry.shape, 1) == 0, column, 0.0)
    out_ref[...] = ry + jnp.where(iota(ry.shape, 0) == 0, jnp.sum(cx, axis=0, keepdims=True), 0.0)


def pair_body(mine_ref, other_ref, out_ref):
    core = lax.rem(lax.axis_index("gy"), 2)
    n = out_ref.shape[0]
    both = mine_ref[...] + other_ref[...]
    out_ref[...] = jnp.where(core == 0, both[:n], both[n:])


def round_body(by, from_ref, own_ref, *refs):
    chip = lax.div(lax.axis_index("gy"), 2)
    got = jnp.where(chip >= by, from_ref[...], 0.0)
    low_refs, (low_out, *own_out) = refs[:-2] if by < 4 else refs[:-1], refs[-2:] if by < 4 else refs[-1:]
    low_out[...] = got + low_refs[0][...] if low_refs else got
    for ref in own_out:
        ref[...] = got + own_ref[...]


def local_body(nb, v_ref, cz_ref, cx_ref, out_ref, acc):
    i = pl.program_id(0)
    ny, nz = acc.shape
    up = upper(nz)

    @pl.when(i == 0)
    def _():
        acc[...] = scan_rows(times(cx_ref[...], up))

    lane = iota((ny, nz), 1)
    cz = cz_ref[...]
    rows = []
    for j in range(nb):
        x = i * nb + j
        rows.append(v_ref[j] + jnp.where(lane == 0, pltpu.roll(cz, lax.rem(nz - x, nz), 1), 0.0))
    along = times(jnp.concatenate(rows, axis=0), up).reshape(nb, ny, nz)
    total = acc[...]
    for j in range(nb):
        total = total + scan_rows(along[j])
        out_ref[j] = total
    acc[...] = total


def local(v, cz, cx):
    nx, ny, nz = v.shape
    nb = 32
    return call(
        functools.partial(local_body, nb),
        [v.shape],
        grid=(nx // nb,),
        ins=[pl.BlockSpec((nb, ny, nz), lambda i: (i, 0, 0)), whole(cz.shape), whole(cx.shape)],
        outs=[pl.BlockSpec((nb, ny, nz), lambda i: (i, 0, 0))],
        scratch=[pltpu.VMEM((ny, nz), F32)],
        flops=1 << 29,
        moved=8 << 20,
    )(v, cz, cx)[0]


def last_body(nb, scale, s_ref, half_ref, other_half_ref, partner_ref, out_ref, gy):
    i = pl.program_id(0)

    @pl.when(i == 0)
    def _():
        core = lax.rem(lax.axis_index("gy"), 2)
        mine, other = half_ref[...], other_half_ref[...]
        cy = jnp.concatenate([jnp.where(core == 0, mine, other), jnp.where(core == 0, other, mine)], axis=0)
        cy = cy + jnp.where(core == 1, partner_ref[...], 0.0)
        gy[...] = times_left(lower(cy.shape[0]), times(cy, upper(cy.shape[1])))

    rows = gy[pl.ds(pl.multiple_of(i * nb, nb), nb), :]
    for j in range(nb):
        out_ref[j] = (s_ref[j] + rows[j : j + 1]) * scale


def last(s, half, other_half, partner, scale):
    nx, ny, nz = s.shape
    nb = 32
    return call(
        functools.partial(last_body, nb, scale),
        [s.shape],
        grid=(nx // nb,),
        ins=[pl.BlockSpec((nb, ny, nz), lambda i: (i, 0, 0)), whole(half.shape), whole(half.shape), whole(partner.shape)],
        outs=[pl.BlockSpec((nb, ny, nz), lambda i: (i, 0, 0))],
        scratch=[pltpu.VMEM((nx, nz), F32)],
        flops=1 << 24,
        moved=8 << 20,
    )(s, half, other_half, partner)[0]


def strips_body(sizes, first_ref, last_ref, lo_a, lo_b, hi_a, hi_b, up_ref, down_ref):
    own = lax.axis_index("gx")
    has_lo, has_hi = own > 0, own < sizes["gx"] - 1
    for v_ref, lo_ref, hi_ref, out_ref, at in ((first_ref, lo_a, hi_a, down_ref, 0), (last_ref, lo_b, hi_b, up_ref, 6)):
        for layer in range(2):
            lo = jnp.where(has_lo, lo_ref[:, at + layer, :], 0.0)
            hi = jnp.where(has_hi, hi_ref[:, at + layer, :], 0.0)
            out_ref[layer] = five_rows(jnp.concatenate([lo, v_ref[:, at + layer, :], hi], axis=0))


def strips(v, x_lo, x_hi, sizes):
    nx, ny, nz = v.shape
    end = ny // 8 - 1
    at_first, at_last = lambda i: (0, 0, 0), lambda i: (0, end, 0)
    return call(
        functools.partial(strips_body, sizes),
        [(2, nx, nz), (2, nx, nz)],
        grid=(1,),
        ins=[
            pl.BlockSpec((nx, 8, nz), at_first),
            pl.BlockSpec((nx, 8, nz), at_last),
            pl.BlockSpec((2, 8, nz), at_first),
            pl.BlockSpec((2, 8, nz), at_last),
            pl.BlockSpec((2, 8, nz), at_first),
            pl.BlockSpec((2, 8, nz), at_last),
        ],
        outs=[whole((2, nx, nz)), whole((2, nx, nz))],
        flops=1 << 22,
        moved=2 << 20,
    )(v, v, x_lo, x_lo, x_hi, x_hi)


def box_xy_body(nb, sizes, v_ref, x_lo, x_hi, y_lo, y_hi, out_ref, up_ref, down_ref):
    i = pl.program_id(0)
    steps = pl.num_programs(0)
    gx, gy = lax.axis_index("gx"), lax.axis_index("gy")
    ny, nz = v_ref.shape[1:]
    base = pl.multiple_of(i * nb, nb)
    group = lax.div(i * nb * 2, nz)

    def run(first, final):
        def row(j):
            if first and j < 0:
                return jnp.where(gx > 0, x_lo[j + 2], 0.0)
            if final and j >= nb:
                return jnp.where(gx < sizes["gx"] - 1, x_hi[j - nb], 0.0)
            return v_ref[base + j]

        lane = iota((ny, nz), 1)
        lows = [jnp.where(gy > 0, y_lo[l, pl.ds(base, nb), :], 0.0) for l in range(2)]
        highs = [jnp.where(gy < sizes["gy"] - 1, y_hi[l, pl.ds(base, nb), :], 0.0) for l in range(2)]
        up = jnp.zeros((ny, nz), F32)
        down = jnp.zeros((ny, nz), F32)
        twos = {j: row(j) + row(j + 1) for j in range(-2, nb + 1)}
        for j in range(nb):
            along = twos[j - 2] + twos[j] + row(j + 2)
            ext = jnp.concatenate(
                [lows[0][j : j + 1], lows[1][j : j + 1], along, highs[0][j : j + 1], highs[1][j : j + 1]], axis=0
            )
            box = five_rows(ext)
            out_ref[j] = box
            at = lax.rem(base + j, nz // 2) * 2
            here = lax.div(lane, 2) * 2 == at
            up = jnp.where(here, pltpu.roll(box, lax.rem(at + 2, nz), 1), up)
            down = jnp.where(here, pltpu.roll(box, at, 1), down)
        at0 = lax.rem(base, nz // 2) * 2
        mine = jnp.logical_and(lane >= at0, lane < at0 + 2 * nb)
        up_ref[group] = jnp.where(mine, up, up_ref[group])
        down_ref[group] = jnp.where(mine, down, down_ref[group])

    pl.when(i == 0)(lambda: run(True, False))
    pl.when(i == steps - 1)(lambda: run(False, True))
    pl.when(jnp.logical_and(i > 0, i < steps - 1))(lambda: run(False, False))


def box_xy(v, x_lo, x_hi, y_lo, y_hi, sizes):
    nx, ny, nz = v.shape
    nb = 32
    packed = (2 * nx // nz, ny, nz)
    return call(
        functools.partial(box_xy_body, nb, sizes),
        [v.shape, packed, packed],
        grid=(nx // nb,),
        ins=[whole(v.shape), whole(x_lo.shape), whole(x_hi.shape), whole(y_lo.shape), whole(y_hi.shape)],
        outs=[pl.BlockSpec((nb, ny, nz), lambda i: (i, 0, 0)), whole(packed), whole(packed)],
        flops=1 << 26,
        moved=8 << 20,
    )(v, x_lo, x_hi, y_lo, y_hi)


def box_z_body(nb, sizes, scale, w_ref, lo_ref, hi_ref, out_ref, lo, hi):
    i = pl.program_id(0)
    gz = lax.axis_index("gz")
    nz = w_ref.shape[2]
    ny = w_ref.shape[1]

    @pl.when(i == 0)
    def _():
        for g in range(lo.shape[0]):
            even = lax.rem(iota((ny, nz), 1), 2) == 0
            a, b = lo_ref[g], hi_ref[g]
            a = a + jnp.where(even, pltpu.roll(a, nz - 1, 1), 0.0)
            b = b + jnp.where(even, 0.0, pltpu.roll(b, 1, 1))
            lo[g] = jnp.where(gz > 0, a, 0.0)
            hi[g] = jnp.where(gz < sizes["gz"] - 1, b, 0.0)

    away = iota((nz, nz), 0) - iota((nz, nz), 1)
    band = ones_where(jnp.logical_and(away <= 2, away >= -2))
    along = times(w_ref[...].reshape(nb * ny, nz), band).reshape(nb, ny, nz)
    lane = iota((ny, nz), 1)
    group = lax.div(i * nb * 2, nz)
    a, b = lo[group], hi[group]
    for j in range(nb):
        at = lax.rem(i * nb + j, nz // 2) * 2
        left = pltpu.roll(a, lax.rem(nz - at, nz), 1)
        right = pltpu.roll(b, lax.rem(2 * nz - 2 - at, nz), 1)
        side = jnp.where(lane < 2, left, jnp.where(lane >= nz - 2, right, 0.0))
        out_ref[j] = (along[j] + side) * scale


def box_z(w, lo, hi, sizes, scale):
    nx, ny, nz = w.shape
    nb = 32
    return call(
        functools.partial(box_z_body, nb, sizes, scale),
        [w.shape],
        grid=(nx // nb,),
        ins=[pl.BlockSpec((nb, ny, nz), lambda i: (i, 0, 0)), whole(lo.shape), whole(hi.shape)],
        outs=[pl.BlockSpec((nb, ny, nz), lambda i: (i, 0, 0))],
        scratch=[pltpu.VMEM(lo.shape, F32), pltpu.VMEM(lo.shape, F32)],
        flops=1 << 29,
        moved=8 << 20,
    )(w, lo, hi)[0]


def shift(v, axis, by):
    n = lax.axis_size(axis)
    return lax.ppermute(v, axis, [(i, (i + by) % n) for i in range(n)])


def partner(v):
    return lax.ppermute(v, "gy", [(i, i ^ 1) for i in range(lax.axis_size("gy"))])


def per_device(v):
    nx, ny, nz = v.shape
    sizes = {a: lax.axis_size(a) for a in ("gx", "gy", "gz")}
    cells = nx * ny * nz * sizes["gx"] * sizes["gy"] * sizes["gz"]

    held, rz, rx, ry = totals(v)

    from_z = [shift(rz, "gz", d) for d in (1, 2, 3)]
    x_lo, x_hi = shift(held[nx - 2 :], "gx", 1), shift(held[:2], "gx", -1)
    cz, rx = call(after_z_body, [rz.shape, rx.shape])(*from_z, rx)

    from_x = [shift(rx, "gx", d) for d in (1, 2, 3)]
    up, down = strips(held, x_lo, x_hi, sizes)
    y_lo, y_hi = shift(up, "gy", 1), shift(down, "gy", -1)
    cx, ry = call(after_x_body, [rx.shape, ry.shape])(*from_x, cz, ry)

    other = partner(ry)
    shape = (nx // 2, nz)
    (half,) = call(pair_body, [shape])(ry, other)
    got = shift(half, "gy", 2)
    w, up, down = box_xy(held, x_lo, x_hi, y_lo, y_hi, sizes)
    low, half = call(functools.partial(round_body, 1), [shape] * 2)(got, half)
    got = shift(half, "gy", 4)
    z_lo, z_hi = shift(up, "gz", 1), shift(down, "gz", -1)
    s = local(held, cz, cx)
    low, half = call(functools.partial(round_body, 2), [shape] * 2)(got, half, low)
    got = shift(half, "gy", 8)
    box_sum = box_z(w, z_lo, z_hi, sizes, 1.0 / math.sqrt(125.0))
    (low,) = call(functools.partial(round_body, 4), [shape])(got, half, low)
    other_low = partner(low)
    prefix = last(s, low, other_low, other, 1.0 / math.sqrt(cells))
    return (prefix, box_sum)


def solution(mesh):
    return jax.shard_map(
        per_device,
        mesh=mesh,
        in_specs=(P("gx", "gy", "gz"),),
        out_specs=(P("gx", "gy", "gz"), P("gx", "gy", "gz")),
        check_vma=False,
    )
```

```python
import functools
import math

import jax
import jax.numpy as jnp
from jax import lax
from jax.experimental import pallas as pl
from jax.experimental.pallas import tpu as pltpu
from jax.sharding import PartitionSpec as P


F32, BF16 = jnp.float32, jnp.bfloat16
MIB = 1 << 20


def iota(shape, dim):
    return lax.broadcasted_iota(jnp.int32, shape, dim)


def split(v):
    high = v.astype(BF16)
    return high, (v - high.astype(F32)).astype(BF16)


def ones_where(keep):
    return jnp.where(keep, 1.0, 0.0).astype(BF16)


def times(v, ones):
    parts, twice = jnp.concatenate(split(v), axis=1), jnp.concatenate([ones, ones], axis=0)
    return jnp.dot(parts, twice, preferred_element_type=F32)


def times_left(ones, v):
    high, low = split(v)
    dot = functools.partial(jnp.dot, preferred_element_type=F32)
    return dot(ones, high) + dot(ones, low)


def upper(n):
    return ones_where(iota((n, n), 0) <= iota((n, n), 1))


def lower(n):
    return ones_where(iota((n, n), 1) <= iota((n, n), 0))


def scan_rows(v):
    dim, n = v.ndim - 2, v.shape[-2]
    step = 1
    while step < n:
        if step < 8:
            moved = jnp.where(iota(v.shape, dim) >= step, pltpu.roll(v, step, dim), 0.0)
        else:
            kept = lax.slice_in_dim(v, 0, n - step, axis=dim)
            moved = jnp.concatenate([jnp.zeros_like(lax.slice_in_dim(v, 0, step, axis=dim)), kept], axis=dim)
        v = v + moved
        step *= 2
    return v


def five_rows(v):
    n = v.shape[0]
    two = v[: n - 1] + v[1:]
    four = two[: n - 3] + two[2:]
    return four[: n - 4] + v[4:]


def cost(flops, moved):
    return pl.CostEstimate(flops=flops, bytes_accessed=moved, transcendentals=0)


def call(body, out, grid=None, ins=None, outs=None, scratch=(), flops=1 << 20, moved=1 << 20, vmem=24):
    shapes = [jax.ShapeDtypeStruct(s, F32) for s in out]
    kw = {}
    if grid is not None:
        kw = dict(grid=grid, in_specs=ins, out_specs=outs)
    return pl.pallas_call(
        body,
        out_shape=shapes,
        scratch_shapes=list(scratch),
        compiler_params=pltpu.CompilerParams(vmem_limit_bytes=vmem * MIB),
        cost_estimate=cost(flops, moved),
        **kw,
    )


def whole(shape):
    return pl.BlockSpec(shape, lambda *_: (0,) * len(shape))


def xy_totals_body(pieces, v_ref, held_ref, rx_ref, ry_ref, near_ref, far_ref, sems):
    nx, ny, nz = held_ref.shape
    n = nx // pieces
    copies = [
        pltpu.make_async_copy(v_ref.at[pl.ds(k * n, n)], held_ref.at[pl.ds(k * n, n)], sems.at[k]) for k in range(pieces)
    ]
    for copy in copies:
        copy.start()

    def group(i, rx):
        rows = []
        for j in range(8):
            v = held_ref[i * 8 + j]
            rx = rx + v
            rows.append(jnp.sum(v, axis=0, keepdims=True))
        ry_ref[pl.ds(pl.multiple_of(i * 8, 8), 8), :] = jnp.concatenate(rows, axis=0)
        return rx

    rx = jnp.zeros((ny, nz), F32)
    for k, copy in enumerate(copies):
        copy.wait()
        rx = lax.fori_loop(k * n // 8, (k + 1) * n // 8, group, rx)
    rx_ref[...] = rx
    near_ref[...], far_ref[...] = facing("gx", held_ref[:2], held_ref[nx - 2 :])


def xy_totals(v):
    nx, ny, nz = v.shape
    pieces = 8
    return pl.pallas_call(
        functools.partial(xy_totals_body, pieces),
        out_shape=[jax.ShapeDtypeStruct(s, F32) for s in (v.shape, (ny, nz), (nx, nz), (2, ny, nz), (2, ny, nz))],
        in_specs=[pl.BlockSpec(memory_space=pltpu.HBM)],
        out_specs=[pl.BlockSpec(memory_space=pltpu.VMEM)] * 5,
        scratch_shapes=[pltpu.SemaphoreType.DMA((pieces,))],
        compiler_params=pltpu.CompilerParams(vmem_limit_bytes=48 * MIB),
        cost_estimate=cost(6 << 20, 8 << 20),
    )(v)


def z_totals_body(v_ref, rz_ref):
    nx, ny, _ = v_ref.shape
    lane = iota((ny, nx), 1)

    def group(i, rz):
        for j in range(8):
            rz = jnp.where(lane == i * 8 + j, jnp.sum(v_ref[i * 8 + j], axis=1, keepdims=True), rz)
        return rz

    rz_ref[...] = lax.fori_loop(0, nx // 8, group, jnp.zeros((ny, nx), F32))


def merge_body(axis, bit, from_ref, own_ref, *refs):
    got = from_ref[...]
    *low_ref, low_out, own_out = refs
    low = jnp.where(lax.rem(lax.shift_right_logical(lax.axis_index(axis), bit), 2) == 1, got, 0.0)
    low_out[...] = low + low_ref[0][...] if low_ref else low
    own_out[...] = own_ref[...] + got


def merge(axis, bit, got, own, *low):
    return call(functools.partial(merge_body, axis, bit), [own.shape] * 2)(got, own, *low)


def high_bit(axis, bit, got_ref, low_ref):
    return low_ref[...] + jnp.where(lax.shift_right_logical(lax.axis_index(axis), bit) == 1, got_ref[...], 0.0)


def spread_body(ry_ref, out_ref):
    ry = ry_ref[...]
    out_ref[...] = times_left(lower(ry.shape[0]), times(ry, upper(ry.shape[1])))


def after_x_body(got_ref, low_ref, rz_ref, cx_ref, out_ref):
    cx = high_bit("gx", 1, got_ref, low_ref)
    cx_ref[...] = cx
    rz = rz_ref[...]
    out_ref[...] = rz + jnp.where(iota(rz.shape, 1) == 0, jnp.sum(cx, axis=1, keepdims=True), 0.0)


def after_z_body(got_ref, low_ref, cx_ref, ry_ref, cz_ref, out_ref):
    cz = high_bit("gz", 1, got_ref, low_ref)
    cz_ref[...] = cz
    nx, nz = ry_ref.shape
    row = jnp.sum(cz, axis=0, keepdims=True)
    column = jnp.sum(jnp.where(iota((nx, nx), 1) <= iota((nx, nx), 0), row, 0.0), axis=1, keepdims=True)
    along = times(jnp.broadcast_to(jnp.sum(cx_ref[...], axis=0, keepdims=True), (8, nz)), upper(nz))
    out_ref[...] = ry_ref[...] + column + along[:1]


def pair_body(mine_ref, other_ref, out_ref):
    core = lax.rem(lax.axis_index("gy"), 2)
    n = out_ref.shape[0]
    both = mine_ref[...] + other_ref[...]
    out_ref[...] = jnp.where(core == 0, both[:n], both[n:])


def after_y_body(got_ref, low_ref, out_ref):
    out_ref[...] = high_bit("gy", 3, got_ref, low_ref)


def local_body(nb, v_ref, cz_ref, cx_ref, out_ref, acc):
    i = pl.program_id(0)
    ny, nz = acc.shape
    up = upper(nz)

    @pl.when(i == 0)
    def _():
        acc[...] = scan_rows(times(cx_ref[...], up))

    lane = iota((ny, nz), 1)
    cz = cz_ref[...]
    rows = []
    for j in range(nb):
        x = i * nb + j
        rows.append(v_ref[j] + jnp.where(lane == 0, pltpu.roll(cz, lax.rem(nz - x, nz), 1), 0.0))
    along = times(jnp.concatenate(rows, axis=0), up).reshape(nb, ny, nz)
    total = acc[...]
    for j in range(nb):
        total = total + scan_rows(along[j])
        out_ref[j] = total
    acc[...] = total


def local(v, cz, cx):
    nx, ny, nz = v.shape
    nb = 32
    return call(
        functools.partial(local_body, nb),
        [v.shape],
        grid=(nx // nb,),
        ins=[pl.BlockSpec((nb, ny, nz), lambda i: (i, 0, 0)), whole(cz.shape), whole(cx.shape)],
        outs=[pl.BlockSpec((nb, ny, nz), lambda i: (i, 0, 0))],
        scratch=[pltpu.VMEM((ny, nz), F32)],
        flops=1 << 29,
        moved=8 << 20,
    )(v, cz, cx)[0]


def last_body(pieces, scale, s_ref, half_ref, other_half_ref, partner_ref, out_ref, gy, made, sems):
    core = lax.rem(lax.axis_index("gy"), 2)
    n = half_ref.shape[0]
    mine, other = half_ref[...], other_half_ref[...]
    for k in range(2):
        part = jnp.where(core == k, mine, other)
        gy[k * n : (k + 1) * n] = part + jnp.where(core == 1, partner_ref[k * n : (k + 1) * n], 0.0)
    n = made.shape[0] // pieces
    copies = []
    for k in range(pieces):

        def group(i, _):
            rows = gy[pl.ds(pl.multiple_of(i * 8, 8), 8), :]
            for j in range(8):
                made[i * 8 + j] = (s_ref[i * 8 + j] + rows[j : j + 1]) * scale
            return 0

        lax.fori_loop(k * n // 8, (k + 1) * n // 8, group, 0)
        copies.append(pltpu.make_async_copy(made.at[pl.ds(k * n, n)], out_ref.at[pl.ds(k * n, n)], sems.at[k]))
        copies[k].start()
    for copy in copies:
        copy.wait()


def last(s, half, other_half, partner, scale):
    nx, _, nz = s.shape
    pieces = 8
    return pl.pallas_call(
        functools.partial(last_body, pieces, scale),
        out_shape=jax.ShapeDtypeStruct(s.shape, F32),
        in_specs=[pl.BlockSpec(memory_space=pltpu.VMEM)] * 4,
        out_specs=pl.BlockSpec(memory_space=pltpu.HBM),
        scratch_shapes=[pltpu.VMEM((nx, nz), F32), pltpu.VMEM(s.shape, F32), pltpu.SemaphoreType.DMA((pieces,))],
        compiler_params=pltpu.CompilerParams(vmem_limit_bytes=24 * MIB),
        cost_estimate=cost(1 << 24, 8 << 20),
    )(s, half, other_half, partner)


def sides(axis, near, far):
    own = lax.axis_index(axis)
    even = lax.rem(own, 2) == 0
    lower = jnp.where(own > 0, jnp.where(even, far, near), 0.0)
    return lower, jnp.where(own < lax.axis_size(axis) - 1, jnp.where(even, near, far), 0.0)


def facing(axis, first, final):
    even = lax.rem(lax.axis_index(axis), 2) == 0
    return jnp.where(even, final, first), jnp.where(even, first, final)


def strips_body(first_ref, last_ref, near_a, far_a, near_b, far_b, near_ref, far_ref):
    for layer in range(2):
        made = []
        for v_ref, near, far, y in ((first_ref, near_a, far_a, layer), (last_ref, near_b, far_b, 6 + layer)):
            lo, hi = sides("gx", near[:, y, :], far[:, y, :])
            made.append(five_rows(jnp.concatenate([lo, v_ref[:, y, :], hi], axis=0)))
        near_ref[layer], far_ref[layer] = facing("gy", *made)


def strips(v, x_near, x_far):
    nx, ny, nz = v.shape
    end = ny // 8 - 1
    at_first, at_last = lambda i: (0, 0, 0), lambda i: (0, end, 0)
    return call(
        strips_body,
        [(2, nx, nz), (2, nx, nz)],
        grid=(1,),
        ins=[
            pl.BlockSpec((nx, 8, nz), at_first),
            pl.BlockSpec((nx, 8, nz), at_last),
            pl.BlockSpec((2, 8, nz), at_first),
            pl.BlockSpec((2, 8, nz), at_first),
            pl.BlockSpec((2, 8, nz), at_last),
            pl.BlockSpec((2, 8, nz), at_last),
        ],
        outs=[whole((2, nx, nz)), whole((2, nx, nz))],
        flops=1 << 22,
        moved=2 << 20,
    )(v, v, x_near, x_far, x_near, x_far)


def box_xy_body(nb, v_ref, x_near, x_far, y_near, y_far, out_ref, near_ref, far_ref):
    i = pl.program_id(0)
    steps = pl.num_programs(0)
    ny, nz = v_ref.shape[1:]
    base = pl.multiple_of(i * nb, nb)
    group = lax.div(i * nb * 2, nz)

    def run(first, final):
        def row(j):
            if first and j < 0:
                return sides("gx", x_near[j + 2], x_far[j + 2])[0]
            if final and j >= nb:
                return sides("gx", x_near[j - nb], x_far[j - nb])[1]
            return v_ref[base + j]

        lane = iota((ny, nz), 1)
        pairs = [sides("gy", y_near[k, pl.ds(base, nb), :], y_far[k, pl.ds(base, nb), :]) for k in range(2)]
        lows, highs = zip(*pairs)
        up = jnp.zeros((ny, nz), F32)
        down = jnp.zeros((ny, nz), F32)
        twos = {j: row(j) + row(j + 1) for j in range(-2, nb + 1)}
        for j in range(nb):
            along = twos[j - 2] + twos[j] + row(j + 2)
            ext = jnp.concatenate(
                [lows[0][j : j + 1], lows[1][j : j + 1], along, highs[0][j : j + 1], highs[1][j : j + 1]], axis=0
            )
            box = five_rows(ext)
            out_ref[j] = box
            at = lax.rem(base + j, nz // 2) * 2
            here = lax.div(lane, 2) * 2 == at
            up = jnp.where(here, pltpu.roll(box, lax.rem(at + 2, nz), 1), up)
            down = jnp.where(here, pltpu.roll(box, at, 1), down)
        at0 = lax.rem(base, nz // 2) * 2
        mine = jnp.logical_and(lane >= at0, lane < at0 + 2 * nb)
        near, far = facing("gz", down, up)
        near_ref[group] = jnp.where(mine, near, near_ref[group])
        far_ref[group] = jnp.where(mine, far, far_ref[group])

    pl.when(i == 0)(lambda: run(True, False))
    pl.when(i == steps - 1)(lambda: run(False, True))
    pl.when(jnp.logical_and(i > 0, i < steps - 1))(lambda: run(False, False))


def box_xy(v, x_near, x_far, y_near, y_far):
    nx, ny, nz = v.shape
    nb = 32
    packed = (2 * nx // nz, ny, nz)
    return call(
        functools.partial(box_xy_body, nb),
        [v.shape, packed, packed],
        grid=(nx // nb,),
        ins=[whole(v.shape), whole(x_near.shape), whole(x_far.shape), whole(y_near.shape), whole(y_far.shape)],
        outs=[pl.BlockSpec((nb, ny, nz), lambda i: (i, 0, 0)), whole(packed), whole(packed)],
        flops=1 << 26,
        moved=8 << 20,
    )(v, x_near, x_far, y_near, y_far)


def box_z_body(nb, scale, w_ref, near_ref, far_ref, out_ref, both):
    i = pl.program_id(0)
    ny, nz = w_ref.shape[1:]
    lane = iota((ny, nz), 1)

    @pl.when(i == 0)
    def _():
        source, target = iota((nz, nz), 0), iota((nz, nz), 1)
        even = lax.rem(lane, 2) == 0
        for g in range(near_ref.shape[0]):
            lo, hi = sides("gz", near_ref[g], far_ref[g])
            lo = lo + jnp.where(even, pltpu.roll(lo, nz - 1, 1), 0.0)
            hi = hi + jnp.where(even, 0.0, pltpu.roll(hi, 1, 1))
            for k in range(2):
                place = lax.div(source, 2) * 4 + lax.rem(source, 2) - k * nz
                both[2 * g + k] = times(hi, ones_where(target == place)) + times(lo, ones_where(target == place + 2))

    away = iota((nz, nz), 0) - iota((nz, nz), 1)
    band = ones_where(jnp.logical_and(away <= 2, away >= -2))
    along = times(w_ref[...].reshape(nb * ny, nz), band).reshape(nb, ny, nz)
    edge = jnp.logical_or(lane < 2, lane >= nz - 2)
    side = both[i]
    for j in range(nb):
        out_ref[j] = (along[j] + jnp.where(edge, pltpu.roll(side, (2 * nz - 2 - 4 * j) % nz, 1), 0.0)) * scale


def box_z(w, near, far, scale):
    nx, ny, nz = w.shape
    nb = nz // 4
    return call(
        functools.partial(box_z_body, nb, scale),
        [w.shape],
        grid=(nx // nb,),
        ins=[pl.BlockSpec((nb, ny, nz), lambda i: (i, 0, 0)), whole(near.shape), whole(far.shape)],
        outs=[pl.BlockSpec((nb, ny, nz), lambda i: (i, 0, 0))],
        scratch=[pltpu.VMEM((nx // nb, ny, nz), F32)],
        flops=1 << 29,
        moved=8 << 20,
    )(w, near, far)[0]


def swap(v, axis, mask):
    return lax.ppermute(v, axis, [(i, i ^ mask) for i in range(lax.axis_size(axis))])


def away(v, axis):
    n = lax.axis_size(axis)
    return lax.ppermute(v, axis, [(i, (i + 2 * (i % 2) - 1) % n) for i in range(n)])


def per_device(v):
    nx, ny, nz = v.shape
    cells = nx * ny * nz * lax.axis_size("gx") * lax.axis_size("gy") * lax.axis_size("gz")

    held, rx, ry, near, far = xy_totals(v)

    got = swap(rx, "gx", 1)
    x_near, x_far = swap(near, "gx", 1), away(far, "gx")
    low, own = merge("gx", 0, got, rx)
    got = swap(own, "gx", 3)
    (rz,) = call(z_totals_body, [(ny, nx)])(held)
    (ry,) = call(spread_body, [ry.shape])(ry)
    cx, rz = call(after_x_body, [rx.shape, rz.shape])(got, low, rz)

    got = swap(rz, "gz", 1)
    near, far = strips(held, x_near, x_far)
    y_near, y_far = swap(near, "gy", 1), away(far, "gy")
    low, own = merge("gz", 0, got, rz)
    got = swap(own, "gz", 3)
    w, near, far = box_xy(held, x_near, x_far, y_near, y_far)
    cz, ry = call(after_z_body, [rz.shape, ry.shape])(got, low, cx, ry)

    other = swap(ry, "gy", 1)
    (own,) = call(pair_body, [(nx // 2, nz)])(ry, other)
    got = swap(own, "gy", 2)
    z_near, z_far = swap(near, "gz", 1), away(far, "gz")
    low, own = merge("gy", 1, got, own)
    got = swap(own, "gy", 6)
    s = local(held, cz, cx)
    low, own = merge("gy", 2, got, own, low)
    got = swap(own, "gy", 14)
    box_sum = box_z(w, z_near, z_far, 1.0 / math.sqrt(125.0))
    (low,) = call(after_y_body, [low.shape])(got, low)
    other_low = swap(low, "gy", 1)
    prefix = last(s, low, other_low, other, 1.0 / math.sqrt(cells))
    return (prefix, box_sum)


def solution(mesh):
    return jax.shard_map(
        per_device,
        mesh=mesh,
        in_specs=(P("gx", "gy", "gz"),),
        out_specs=(P("gx", "gy", "gz"), P("gx", "gy", "gz")),
        check_vma=False,
    )
```

```python
import functools
import math

import jax
import jax.numpy as jnp
from jax import lax
from jax.experimental import pallas as pl
from jax.experimental.pallas import tpu as pltpu
from jax.sharding import PartitionSpec as P


F32, BF16 = jnp.float32, jnp.bfloat16
MIB = 1 << 20


def iota(shape, dim):
    return lax.broadcasted_iota(jnp.int32, shape, dim)


def split(v):
    high = v.astype(BF16)
    return high, (v - high.astype(F32)).astype(BF16)


def ones_where(keep):
    return jnp.where(keep, 1.0, 0.0).astype(BF16)


def times(v, ones):
    parts, twice = jnp.concatenate(split(v), axis=1), jnp.concatenate([ones, ones], axis=0)
    return jnp.dot(parts, twice, preferred_element_type=F32)


def times_left(ones, v):
    high, low = split(v)
    dot = functools.partial(jnp.dot, preferred_element_type=F32)
    return dot(ones, high) + dot(ones, low)


def upper(n):
    return ones_where(iota((n, n), 0) <= iota((n, n), 1))


def lower(n):
    return ones_where(iota((n, n), 1) <= iota((n, n), 0))


def scan_rows(v):
    dim, n = v.ndim - 2, v.shape[-2]
    step = 1
    while step < n:
        if step < 8:
            moved = jnp.where(iota(v.shape, dim) >= step, pltpu.roll(v, step, dim), 0.0)
        else:
            kept = lax.slice_in_dim(v, 0, n - step, axis=dim)
            moved = jnp.concatenate([jnp.zeros_like(lax.slice_in_dim(v, 0, step, axis=dim)), kept], axis=dim)
        v = v + moved
        step *= 2
    return v


def five_rows(v):
    n = v.shape[0]
    two = v[: n - 1] + v[1:]
    four = two[: n - 3] + two[2:]
    return four[: n - 4] + v[4:]


def cost(flops, moved):
    return pl.CostEstimate(flops=flops, bytes_accessed=moved, transcendentals=0)


def call(body, out, grid=None, ins=None, outs=None, scratch=(), flops=1 << 20, moved=1 << 20, vmem=24):
    shapes = [jax.ShapeDtypeStruct(s, F32) for s in out]
    kw = {}
    if grid is not None:
        kw = dict(grid=grid, in_specs=ins, out_specs=outs)
    return pl.pallas_call(
        body,
        out_shape=shapes,
        scratch_shapes=list(scratch),
        compiler_params=pltpu.CompilerParams(vmem_limit_bytes=vmem * MIB),
        cost_estimate=cost(flops, moved),
        **kw,
    )


def whole(shape):
    return pl.BlockSpec(shape, lambda *_: (0,) * len(shape))


def xy_totals_body(pieces, v_ref, held_ref, rx_ref, ry_ref, near_ref, far_ref, sems):
    nx, ny, nz = held_ref.shape
    n = nx // pieces
    copies = [
        pltpu.make_async_copy(v_ref.at[pl.ds(k * n, n)], held_ref.at[pl.ds(k * n, n)], sems.at[k]) for k in range(pieces)
    ]
    for copy in copies:
        copy.start()

    def group(i, rx):
        rows = []
        for j in range(8):
            v = held_ref[i * 8 + j]
            rx = rx + v
            rows.append(jnp.sum(v, axis=0, keepdims=True))
        ry_ref[pl.ds(pl.multiple_of(i * 8, 8), 8), :] = jnp.concatenate(rows, axis=0)
        return rx

    rx = jnp.zeros((ny, nz), F32)
    for k, copy in enumerate(copies):
        copy.wait()
        rx = lax.fori_loop(k * n // 8, (k + 1) * n // 8, group, rx)
    rx_ref[...] = rx
    near_ref[...], far_ref[...] = facing("gx", held_ref[:2], held_ref[nx - 2 :])


def xy_totals(v):
    nx, ny, nz = v.shape
    pieces = 8
    return pl.pallas_call(
        functools.partial(xy_totals_body, pieces),
        out_shape=[jax.ShapeDtypeStruct(s, F32) for s in (v.shape, (ny, nz), (nx, nz), (2, ny, nz), (2, ny, nz))],
        in_specs=[pl.BlockSpec(memory_space=pltpu.HBM)],
        out_specs=[pl.BlockSpec(memory_space=pltpu.VMEM)] * 5,
        scratch_shapes=[pltpu.SemaphoreType.DMA((pieces,))],
        compiler_params=pltpu.CompilerParams(vmem_limit_bytes=48 * MIB),
        cost_estimate=cost(6 << 20, 8 << 20),
    )(v)


def z_totals_body(v_ref, rz_ref):
    nx, ny, _ = v_ref.shape
    lane = iota((ny, nx), 1)

    def group(i, rz):
        for j in range(8):
            rz = jnp.where(lane == i * 8 + j, jnp.sum(v_ref[i * 8 + j], axis=1, keepdims=True), rz)
        return rz

    rz_ref[...] = lax.fori_loop(0, nx // 8, group, jnp.zeros((ny, nx), F32))


def merge_body(axis, bit, from_ref, own_ref, *refs):
    got = from_ref[...]
    *low_ref, low_out, own_out = refs
    low = jnp.where(lax.rem(lax.shift_right_logical(lax.axis_index(axis), bit), 2) == 1, got, 0.0)
    low_out[...] = low + low_ref[0][...] if low_ref else low
    own_out[...] = own_ref[...] + got


def merge(axis, bit, got, own, *low):
    return call(functools.partial(merge_body, axis, bit), [own.shape] * 2)(got, own, *low)


def high_bit(axis, bit, got_ref, low_ref):
    return low_ref[...] + jnp.where(lax.shift_right_logical(lax.axis_index(axis), bit) == 1, got_ref[...], 0.0)


def spread_body(ry_ref, out_ref):
    ry = ry_ref[...]
    out_ref[...] = times_left(lower(ry.shape[0]), times(ry, upper(ry.shape[1])))


def after_x_body(got_ref, low_ref, rz_ref, cx_ref, out_ref):
    cx = high_bit("gx", 1, got_ref, low_ref)
    cx_ref[...] = cx
    rz = rz_ref[...]
    out_ref[...] = rz + jnp.where(iota(rz.shape, 1) == 0, jnp.sum(cx, axis=1, keepdims=True), 0.0)


def after_z_body(got_ref, low_ref, cx_ref, ry_ref, cz_ref, out_ref):
    cz = high_bit("gz", 1, got_ref, low_ref)
    cz_ref[...] = cz
    nx, nz = ry_ref.shape
    row = jnp.sum(cz, axis=0, keepdims=True)
    column = jnp.sum(jnp.where(iota((nx, nx), 1) <= iota((nx, nx), 0), row, 0.0), axis=1, keepdims=True)
    along = times(jnp.broadcast_to(jnp.sum(cx_ref[...], axis=0, keepdims=True), (8, nz)), upper(nz))
    out_ref[...] = ry_ref[...] + column + along[:1]


def pair_body(mine_ref, other_ref, out_ref):
    core = lax.rem(lax.axis_index("gy"), 2)
    n = out_ref.shape[0]
    both = mine_ref[...] + other_ref[...]
    out_ref[...] = jnp.where(core == 0, both[:n], both[n:])


def after_y_body(got_ref, low_ref, out_ref):
    out_ref[...] = high_bit("gy", 3, got_ref, low_ref)


def local_body(nb, v_ref, cz_ref, cx_ref, out_ref):
    nx, ny, nz = v_ref.shape
    up = upper(nz)
    lane = iota((ny, nz), 1)

    def block(i, total):
        cz = cz_ref[...]
        rows = []
        for j in range(nb):
            x = i * nb + j
            rows.append(v_ref[x] + jnp.where(lane == 0, pltpu.roll(cz, lax.rem(nz - x, nz), 1), 0.0))
        along = times(jnp.concatenate(rows, axis=0), up).reshape(nb, ny, nz)
        for j in range(nb):
            total = total + scan_rows(along[j])
            out_ref[i * nb + j] = total
        return total

    lax.fori_loop(0, nx // nb, block, scan_rows(times(cx_ref[...], up)))


def local(v, cz, cx):
    nb = 32
    return call(functools.partial(local_body, nb), [v.shape], flops=1 << 29, moved=8 << 20)(v, cz, cx)[0]


def finish_body(pieces, own, scale, s_ref, half_ref, partner_ref, *refs):
    out_ref, made, sems = refs[-3:]
    core = lax.rem(lax.axis_index("gy"), 2)
    n = half_ref.shape[0]
    at = n * (core if own else 1 - core)
    step = n // pieces

    def copy(k):
        rows = pl.ds(k * step, step)
        return pltpu.make_async_copy(made.at[rows], out_ref.at[pl.ds(at + k * step, step)], sems.at[k])

    for k in range(pieces):

        def group(i, _):
            theirs = partner_ref[pl.ds(pl.multiple_of(at + i * 8, 8), 8), :]
            rows = half_ref[pl.ds(pl.multiple_of(i * 8, 8), 8), :] + jnp.where(core == 1, theirs, 0.0)
            for j in range(8):
                made[i * 8 + j] = (s_ref[at + i * 8 + j] + rows[j : j + 1]) * scale
            return 0

        lax.fori_loop(k * step // 8, (k + 1) * step // 8, group, 0)
        copy(k).start()
    for k in range(pieces):
        copy(k).wait()


def finish(s, half, partner, scale, *begun):
    nx, ny, nz = s.shape
    pieces = 8
    return pl.pallas_call(
        functools.partial(finish_body, pieces, not begun, scale),
        out_shape=jax.ShapeDtypeStruct(s.shape, F32),
        in_specs=[pl.BlockSpec(memory_space=pltpu.VMEM)] * 3 + [pl.BlockSpec(memory_space=pltpu.HBM)] * len(begun),
        out_specs=pl.BlockSpec(memory_space=pltpu.HBM),
        scratch_shapes=[pltpu.VMEM((nx // 2, ny, nz), F32), pltpu.SemaphoreType.DMA((pieces,))],
        input_output_aliases={3: 0} if begun else {},
        compiler_params=pltpu.CompilerParams(vmem_limit_bytes=24 * MIB),
        cost_estimate=cost(1 << 23, 4 << 20),
    )(s, half, partner, *begun)


def sides(axis, near, far):
    own = lax.axis_index(axis)
    even = lax.rem(own, 2) == 0
    lower = jnp.where(own > 0, jnp.where(even, far, near), 0.0)
    return lower, jnp.where(own < lax.axis_size(axis) - 1, jnp.where(even, near, far), 0.0)


def facing(axis, first, final):
    even = lax.rem(lax.axis_index(axis), 2) == 0
    return jnp.where(even, final, first), jnp.where(even, first, final)


def strips_body(first_ref, last_ref, near_a, far_a, near_b, far_b, near_ref, far_ref):
    for layer in range(2):
        made = []
        for v_ref, near, far, y in ((first_ref, near_a, far_a, layer), (last_ref, near_b, far_b, 6 + layer)):
            lo, hi = sides("gx", near[:, y, :], far[:, y, :])
            made.append(five_rows(jnp.concatenate([lo, v_ref[:, y, :], hi], axis=0)))
        near_ref[layer], far_ref[layer] = facing("gy", *made)


def strips(v, x_near, x_far):
    nx, ny, nz = v.shape
    end = ny // 8 - 1
    at_first, at_last = lambda i: (0, 0, 0), lambda i: (0, end, 0)
    return call(
        strips_body,
        [(2, nx, nz), (2, nx, nz)],
        grid=(1,),
        ins=[
            pl.BlockSpec((nx, 8, nz), at_first),
            pl.BlockSpec((nx, 8, nz), at_last),
            pl.BlockSpec((2, 8, nz), at_first),
            pl.BlockSpec((2, 8, nz), at_first),
            pl.BlockSpec((2, 8, nz), at_last),
            pl.BlockSpec((2, 8, nz), at_last),
        ],
        outs=[whole((2, nx, nz)), whole((2, nx, nz))],
        flops=1 << 22,
        moved=2 << 20,
    )(v, v, x_near, x_far, x_near, x_far)


def box_xy_body(nb, v_ref, x_near, x_far, y_near, y_far, out_ref, near_ref, far_ref):
    ny, nz = v_ref.shape[1:]
    steps = v_ref.shape[0] // nb

    def run(i, first, final):
        base = pl.multiple_of(i * nb, nb)
        group = lax.div(i * nb * 2, nz)

        def row(j):
            if first and j < 0:
                return sides("gx", x_near[j + 2], x_far[j + 2])[0]
            if final and j >= nb:
                return sides("gx", x_near[j - nb], x_far[j - nb])[1]
            return v_ref[base + j]

        lane = iota((ny, nz), 1)
        pairs = [sides("gy", y_near[k, pl.ds(base, nb), :], y_far[k, pl.ds(base, nb), :]) for k in range(2)]
        lows, highs = zip(*pairs)
        up = jnp.zeros((ny, nz), F32)
        down = jnp.zeros((ny, nz), F32)
        twos = {j: row(j) + row(j + 1) for j in range(-2, nb + 1)}
        for j in range(nb):
            along = twos[j - 2] + twos[j] + row(j + 2)
            ext = jnp.concatenate(
                [lows[0][j : j + 1], lows[1][j : j + 1], along, highs[0][j : j + 1], highs[1][j : j + 1]], axis=0
            )
            box = five_rows(ext)
            out_ref[base + j] = box
            at = lax.rem(base + j, nz // 2) * 2
            here = lax.div(lane, 2) * 2 == at
            up = jnp.where(here, pltpu.roll(box, lax.rem(at + 2, nz), 1), up)
            down = jnp.where(here, pltpu.roll(box, at, 1), down)
        at0 = lax.rem(base, nz // 2) * 2
        mine = jnp.logical_and(lane >= at0, lane < at0 + 2 * nb)
        near, far = facing("gz", down, up)
        near_ref[group] = jnp.where(mine, near, near_ref[group])
        far_ref[group] = jnp.where(mine, far, far_ref[group])

    def inner(i, _):
        run(i, False, False)
        return 0

    run(jnp.int32(0), True, False)
    lax.fori_loop(1, steps - 1, inner, 0)
    run(jnp.int32(steps - 1), False, True)


def box_xy(v, x_near, x_far, y_near, y_far):
    nx, ny, nz = v.shape
    nb = 32
    packed = (2 * nx // nz, ny, nz)
    return call(
        functools.partial(box_xy_body, nb), [v.shape, packed, packed], flops=1 << 26, moved=8 << 20
    )(v, x_near, x_far, y_near, y_far)


def box_z_body(scale, w_ref, near_ref, far_ref, out_ref, both, made, sems):
    nx, ny, nz = w_ref.shape
    nb = nz // 4
    lane = iota((ny, nz), 1)
    source, target = iota((nz, nz), 0), iota((nz, nz), 1)
    even = lax.rem(lane, 2) == 0
    for g in range(near_ref.shape[0]):
        lo, hi = sides("gz", near_ref[g], far_ref[g])
        lo = lo + jnp.where(even, pltpu.roll(lo, nz - 1, 1), 0.0)
        hi = hi + jnp.where(even, 0.0, pltpu.roll(hi, 1, 1))
        for k in range(2):
            place = lax.div(source, 2) * 4 + lax.rem(source, 2) - k * nz
            both[2 * g + k] = times(hi, ones_where(target == place)) + times(lo, ones_where(target == place + 2))

    away = iota((nz, nz), 0) - iota((nz, nz), 1)
    band = ones_where(jnp.logical_and(away <= 2, away >= -2))
    edge = jnp.logical_or(lane < 2, lane >= nz - 2)

    def copy(i):
        at = pl.ds(i * nb, nb)
        return pltpu.make_async_copy(made.at[at], out_ref.at[at], sems.at[i])

    def block(i, _):
        along = times(w_ref[pl.ds(i * nb, nb)].reshape(nb * ny, nz), band).reshape(nb, ny, nz)
        side = both[i]
        for j in range(nb):
            lacking = jnp.where(edge, pltpu.roll(side, (2 * nz - 2 - 4 * j) % nz, 1), 0.0)
            made[i * nb + j] = (along[j] + lacking) * scale
        copy(i).start()
        return 0

    lax.fori_loop(0, nx // nb, block, 0)
    for i in range(nx // nb):
        copy(i).wait()


def box_z(w, near, far, scale):
    nx, ny, nz = w.shape
    steps = 4 * nx // nz
    return pl.pallas_call(
        functools.partial(box_z_body, scale),
        out_shape=jax.ShapeDtypeStruct(w.shape, F32),
        in_specs=[pl.BlockSpec(memory_space=pltpu.VMEM)] * 3,
        out_specs=pl.BlockSpec(memory_space=pltpu.HBM),
        scratch_shapes=[
            pltpu.VMEM((steps, ny, nz), F32),
            pltpu.VMEM(w.shape, F32),
            pltpu.SemaphoreType.DMA((steps,)),
        ],
        compiler_params=pltpu.CompilerParams(vmem_limit_bytes=24 * MIB),
        cost_estimate=cost(1 << 29, 8 << 20),
    )(w, near, far)


def swap(v, axis, mask):
    return lax.ppermute(v, axis, [(i, i ^ mask) for i in range(lax.axis_size(axis))])


def away(v, axis):
    n = lax.axis_size(axis)
    return lax.ppermute(v, axis, [(i, (i + 2 * (i % 2) - 1) % n) for i in range(n)])


def per_device(v):
    nx, ny, nz = v.shape
    cells = nx * ny * nz * lax.axis_size("gx") * lax.axis_size("gy") * lax.axis_size("gz")

    held, rx, ry, near, far = xy_totals(v)

    got = swap(rx, "gx", 1)
    x_far = away(far, "gx")
    low, own = merge("gx", 0, got, rx)
    got = swap(own, "gx", 3)
    x_near = swap(near, "gx", 1)
    (rz,) = call(z_totals_body, [(ny, nx)])(held)
    (ry,) = call(spread_body, [ry.shape])(ry)
    cx, rz = call(after_x_body, [rx.shape, rz.shape])(got, low, rz)

    got = swap(rz, "gz", 1)
    near, far = strips(held, x_near, x_far)
    y_near, y_far = swap(near, "gy", 1), away(far, "gy")
    low, own = merge("gz", 0, got, rz)
    got = swap(own, "gz", 3)
    w, near, far = box_xy(held, x_near, x_far, y_near, y_far)
    cz, ry = call(after_z_body, [rz.shape, ry.shape])(got, low, cx, ry)

    other = swap(ry, "gy", 1)
    (own,) = call(pair_body, [(nx // 2, nz)])(ry, other)
    got = swap(own, "gy", 2)
    z_near, z_far = swap(near, "gz", 1), away(far, "gz")
    low, own = merge("gy", 1, got, own)
    got = swap(own, "gy", 6)
    s = local(held, cz, cx)
    low, own = merge("gy", 2, got, own, low)
    got = swap(own, "gy", 14)
    box_sum = box_z(w, z_near, z_far, 1.0 / math.sqrt(125.0))
    (low,) = call(after_y_body, [low.shape])(got, low)
    other_low = swap(low, "gy", 1)
    scale = 1.0 / math.sqrt(cells)
    prefix = finish(s, low, other, scale)
    prefix = finish(s, other_low, other, scale, prefix)
    return (prefix, box_sum)


def solution(mesh):
    return jax.shard_map(
        per_device,
        mesh=mesh,
        in_specs=(P("gx", "gy", "gz"),),
        out_specs=(P("gx", "gy", "gz"), P("gx", "gy", "gz")),
        check_vma=False,
    )
```
